32 devices in a mesh: row: 4 (over z), col: 8 (over y, x, core).
Axes of the slice: x: 2, y: 2, z: 4, core: 2. Of those that a mesh axis runs over, the one named last changes fastest.
Arguments:
- losses: float32 [8, 16384], P(None, ('row', 'col')), may hold values from 0.05 to 12
- domains: int32 [8, 16384], P(None, ('row', 'col')), may hold values from 0 to 2047
Outputs:
- token_count: float32 [8, 2048], replicated
- loss_mean: float32 [8, 2048], replicated
- loss_variance: float32 [8, 2048], replicated
The draws below stay inside these ranges and needn't reach their ends.
All inputs are finite; a program needn't handle non-finite values.
Results may differ from the reference program's by a relative error of at most 0.0001.
Values sent between devices are 32-bit elements; how exact they have to be, the bound alone decides.
A program may use at most 64 MiB of HBM per device.

```python
import math
import jax
import jax.numpy as jnp
import numpy as np
from jax import lax

DOMAINS = 2048
MICRO = 8
TOKENS = 16384


def touch_ends(result, rng, smallest, high):
    spot = [jax.random.randint(jax.random.fold_in(rng, axis), (), 0, length) for axis, length in enumerate(result.shape)]
    widest = result.shape.index(max(result.shape))
    next_to = spot[:widest] + [(spot[widest] + 1) % result.shape[widest]] + spot[widest + 1:]
    return result.at[tuple(spot)].set(smallest).at[tuple(next_to)].set(high)


def block_scale(key, dims, shards, low, largest):
    def one(dim, shards_of):
        steps = jax.random.uniform(jax.random.fold_in(jax.random.fold_in(key, 6), dim), (shards_of,), jnp.float32, low / len(shards), largest / len(shards))
        return jnp.repeat(jnp.exp(steps), dims[dim] // shards_of).reshape((-1,) + (1,) * (len(dims) - dim - 1))

    level = one(*shards[0])
    for cut in shards[1:]:
        level = level * one(*cut)
    return level


def rank_table(amount, slope):
    weights = [(1 << 20) // math.isqrt(rank ** slope) + 1 for rank in range(1, amount + 1)]
    scale = 1 + sum(weights) // (1 << 30)
    return np.cumsum(np.array([max(1, weight // scale) for weight in weights]))


def skewed_ids(stream_key, extent, amount, skew):
    listing = rank_table(amount, skew)
    lot = jax.random.randint(jax.random.fold_in(stream_key, 1), extent, 0, int(listing[amount - 1]))
    standing = jnp.searchsorted(jnp.asarray(listing, jnp.int32), lot, side="right")
    return jax.random.permutation(jax.random.fold_in(stream_key, 2), amount)[standing].astype(jnp.int32)


def setup_inputs(seed: int = 0) -> dict:
    streams_of = jax.random.split(jax.random.key(seed), 3)
    losses = jnp.clip(jnp.exp(math.log(12.0) - 5.480639 * jax.random.uniform(streams_of[0], (MICRO, TOKENS), jnp.float32) ** block_scale(streams_of[0], (MICRO, TOKENS), ((1, 32),), -0.2, 0.2)), 0.05, 12.0)
    domains = touch_ends(skewed_ids(streams_of[1], (MICRO, TOKENS), DOMAINS, 2), jax.random.fold_in(streams_of[1], 3), 0, DOMAINS - 1).astype(jnp.int32)
    return {"losses": losses, "domains": domains}


def reference(losses, domains):
    offsets = domains + DOMAINS * lax.broadcasted_iota(jnp.int32, domains.shape, 0)
    flat_ids = offsets.reshape(-1).astype(jnp.int32)
    flat_loss = losses.reshape(-1)
    segments = MICRO * DOMAINS
    token_count = jax.ops.segment_sum(jnp.ones_like(flat_loss), flat_ids, segments)
    total = jax.ops.segment_sum(flat_loss, flat_ids, segments)
    loss_mean = total / jnp.maximum(token_count, 1.0)
    deviation = flat_loss - loss_mean[flat_ids]
    spread = jax.ops.segment_sum(deviation * deviation, flat_ids, segments)
    loss_variance = spread / jnp.maximum(token_count - 1.0, 1.0)
    return (token_count.reshape(MICRO, DOMAINS), loss_mean.reshape(MICRO, DOMAINS), loss_variance.reshape(MICRO, DOMAINS))
```

```python
import functools

import jax
import jax.numpy as jnp
from jax import lax
from jax.experimental import pallas as pl
from jax.experimental.pallas import tpu as pltpu
from jax.sharding import PartitionSpec as P

DOMAINS = 2048
LANES = 128
MESH = pl.DeviceIdType.MESH


def pieces(value):
    first = value.astype(jnp.bfloat16).astype(jnp.float32)
    rest = value - first
    second = rest.astype(jnp.bfloat16).astype(jnp.float32)
    return first, second, rest - second


def nt_dot(a, b):
    return lax.dot_general(a, b, (((1,), (1,)), ((), ())), preferred_element_type=jnp.float32)


def local_stats(loss, ids, groups):
    tokens = loss.shape[1]
    low = lax.bitwise_and(ids, LANES - 1)
    high = lax.shift_right_logical(ids, LANES.bit_length() - 1)
    low_hot = (lax.broadcasted_iota(jnp.int32, (LANES, tokens), 0) == low).astype(jnp.float32).astype(jnp.bfloat16)
    in_group = lax.broadcasted_iota(jnp.int32, (groups, tokens), 0) == high

    def spread_out(row):
        return jnp.where(in_group, row, 0.0).astype(jnp.bfloat16)

    first = jnp.concatenate([spread_out(row) for row in (jnp.ones_like(loss),) + pieces(loss)], axis=0)
    sums = nt_dot(first, low_hot)
    count = sums[:groups]
    total = sums[groups:2 * groups] + sums[2 * groups:3 * groups] + sums[3 * groups:]
    mean = total / jnp.maximum(count, 1.0)
    parts = jnp.concatenate([part.astype(jnp.bfloat16) for part in pieces(mean)], axis=0)
    looked = jnp.dot(parts, low_hot, preferred_element_type=jnp.float32)
    looked = looked[:groups] + looked[groups:2 * groups] + looked[2 * groups:]
    centre = jnp.sum(jnp.where(in_group, looked, 0.0), axis=0, keepdims=True)
    deviation = loss - centre
    squares = jnp.concatenate([spread_out(row) for row in pieces(deviation * deviation)], axis=0)
    sums = nt_dot(squares, low_hot)
    spread = sums[:groups] + sums[groups:2 * groups] + sums[2 * groups:]
    return count, total, spread


def kernel(
    axes, sizes, owners, rows, loss_ref, ids_ref, count_ref, mean_ref, variance_ref,
    send, recv, final, send_sem, recv_sem, out_sem, final_sem,
):
    n = sizes[0] * sizes[1]
    micro = loss_ref.shape[0]
    groups = DOMAINS // LANES
    me = lax.axis_index(axes[0]) * sizes[1] + lax.axis_index(axes[1])

    def coordinates(device):
        return (device // sizes[1], device % sizes[1])

    def other(step):
        return lax.rem(me + step, n)

    barrier = pltpu.get_barrier_semaphore()

    @pl.loop(1, n)
    def _(step):
        pl.semaphore_signal(barrier, inc=1, device_id=coordinates(other(step)), device_id_type=MESH)

    for m in range(micro):
        stats = local_stats(loss_ref[m:m + 1, :], ids_ref[m:m + 1, :], groups)
        for part in range(groups // rows):
            owner = m * (groups // rows) + part
            for which, stat in enumerate(stats):
                send[owner, which * rows:(which + 1) * rows, :] = stat[part * rows:(part + 1) * rows]

    pl.semaphore_wait(barrier, n - 1)

    def to_owner(device):
        return pltpu.make_async_remote_copy(
            src_ref=send.at[device], dst_ref=recv.at[me],
            send_sem=send_sem.at[device], recv_sem=recv_sem.at[me],
            device_id=coordinates(device), device_id_type=MESH,
        )

    def from_device(device):
        return pltpu.make_async_remote_copy(
            src_ref=recv.at[device], dst_ref=recv.at[device],
            send_sem=recv_sem.at[device], recv_sem=recv_sem.at[device],
            device_id=coordinates(device), device_id_type=MESH,
        )

    def to_everyone(device):
        return pltpu.make_async_remote_copy(
            src_ref=final.at[me], dst_ref=final.at[me],
            send_sem=out_sem.at[device], recv_sem=final_sem.at[me],
            device_id=coordinates(device), device_id_type=MESH,
        )

    def from_owner(device):
        return pltpu.make_async_remote_copy(
            src_ref=final.at[device], dst_ref=final.at[device],
            send_sem=final_sem.at[device], recv_sem=final_sem.at[device],
            device_id=coordinates(device), device_id_type=MESH,
        )

    def if_owner(device, action):
        if owners == n:
            action()
        else:
            pl.when(device < owners)(action)

    @pl.loop(1, n)
    def _(step):
        device = other(step)
        if_owner(device, lambda: to_owner(device).start())

    def combine():
        recv[me] = send[me]

        @pl.loop(1, n)
        def _(step):
            from_device(other(step)).wait_recv()

        counts = recv[:, :rows, :]
        totals = recv[:, rows:2 * rows, :]
        count = jnp.sum(counts, axis=0)
        mean = jnp.sum(totals, axis=0) / jnp.maximum(count, 1.0)
        gap = totals / jnp.maximum(counts, 1.0) - mean[None]
        spread = jnp.sum(recv[:, 2 * rows:, :] + counts * (gap * gap), axis=0)
        final[me, :rows, :] = count
        final[me, rows:2 * rows, :] = mean
        final[me, 2 * rows:, :] = spread / jnp.maximum(count - 1.0, 1.0)

        @pl.loop(1, n)
        def _(step):
            to_everyone(other(step)).start()

    if_owner(me, combine)

    @pl.loop(1, n)
    def _(step):
        device = other(step)
        if_owner(device, lambda: from_owner(device).wait_recv())

    stride = groups // rows
    for which, out in enumerate((count_ref, mean_ref, variance_ref)):
        for group in range(groups):
            row = which * rows + group % rows
            block = [final[m * stride + group // rows, row:row + 1, :] for m in range(micro)]
            out[:, group * LANES:(group + 1) * LANES] = jnp.concatenate(block, axis=0)

    @pl.loop(1, n)
    def _(step):
        device = other(step)
        if_owner(device, lambda: to_owner(device).wait_send())
        if_owner(me, lambda: to_everyone(device).wait_send())


def solution(mesh):
    axes = tuple(mesh.axis_names)
    sizes = tuple(mesh.shape[axis] for axis in axes)
    n = sizes[0] * sizes[1]

    def on_device(losses, domains):
        micro = losses.shape[0]
        all_rows = micro * (DOMAINS // LANES)
        rows = max(1, all_rows // n)
        owners = all_rows // rows
        out = jax.ShapeDtypeStruct((micro, DOMAINS), jnp.float32)
        return pl.pallas_call(
            functools.partial(kernel, axes, sizes, owners, rows),
            out_shape=(out, out, out),
            in_specs=[pl.BlockSpec(memory_space=pltpu.VMEM)] * 2,
            out_specs=[pl.BlockSpec(memory_space=pltpu.VMEM)] * 3,
            scratch_shapes=[
                pltpu.VMEM((owners, 3 * rows, LANES), jnp.float32),
                pltpu.VMEM((n, 3 * rows, LANES), jnp.float32),
                pltpu.VMEM((owners, 3 * rows, LANES), jnp.float32),
                pltpu.SemaphoreType.DMA((owners,)),
                pltpu.SemaphoreType.DMA((n,)),
                pltpu.SemaphoreType.DMA((n,)),
                pltpu.SemaphoreType.DMA((owners,)),
            ],
            compiler_params=pltpu.CompilerParams(collective_id=0, has_side_effects=True),
        )(losses, domains)

    return jax.shard_map(
        on_device,
        mesh=mesh,
        in_specs=(P(None, axes), P(None, axes)),
        out_specs=(P(), P(), P()),
        check_vma=False,
    )
```
